32 devices in a mesh: gz: 4 (over x, core), gx: 4 (over z), gy: 2 (over y).
Axes of the slice: x: 2, y: 2, z: 4, core: 2. Of those that a mesh axis runs over, the one named last changes fastest.
Arguments:
- offsets: float32 [3, 4, 8, 8, 128], P(None, 'gz', 'gx', 'gy'), may hold values from 0 to 10
- type_ids: int32 [4, 8, 8, 128], P('gz', 'gx', 'gy'), may hold values from 0 to 2
- occupied: int32 [4, 8, 8, 128], P('gz', 'gx', 'gy'), may hold values from 0 to 1, as said below
- prior_charges: float32 [2, 4, 8, 8, 128], P(None, 'gz', 'gx', 'gy'), may hold values from -0.6 to 0.6
- electronegativity: float32 [3], replicated, may hold values from 2 to 10
- hardness: float32 [3], replicated, may hold values from 4 to 12
- shielding: float32 [3], replicated, may hold values from 0.5 to 1.2
Outputs:
- charges: float32 [4, 8, 8, 128], P('gz', 'gx', 'gy')
- residuals: float32 [2, 4, 8, 8, 128], P(None, 'gz', 'gx', 'gy')
The draws below stay inside these ranges and needn't reach their ends.
Inputs may be any that keep to these rules, and one draw needn't show every extreme that they name: `occupied`: 1 marks a slot that holds an atom, 0 a padding slot.
All inputs are finite; a program needn't handle non-finite values.
Results may differ from the reference program's by a relative error of at most 0.00021.
Values sent between devices are 32-bit elements; how exact they have to be, the bound alone decides.
A program may use at most 128 MiB of HBM per device.

```python
import jax
import jax.numpy as jnp
from jax import lax

SLOTS = 128
ITERS = 4
NTYPES = 3
NCZ = 4
NCX = 8
NCY = 8


def draw_occupied(key, part):
    shape = (NCZ, NCX, NCY, SLOTS)
    layer = jnp.arange(NCZ, dtype=jnp.int32)[:, None, None, None]
    threshold = 250 + 700 * layer // max(NCZ - 1, 1)
    rolled = jax.random.randint(jax.random.fold_in(key, 17), shape, 0, 1000)
    return (rolled < threshold).astype(jnp.int32)


def place_ends(entries, rng, smallest, high):
    place = [jax.random.randint(jax.random.fold_in(rng, axis), (), 0, length) for axis, length in enumerate(entries.shape)]
    longest = entries.shape.index(max(entries.shape))
    neighbour = place[:longest] + [(place[longest] + 1) % entries.shape[longest]] + place[longest + 1:]
    return entries.at[tuple(place)].set(smallest).at[tuple(neighbour)].set(high)


def levels(stream_key, shape, shards, least, top_value):
    def one(dim, blocks):
        heights = jax.random.uniform(jax.random.fold_in(jax.random.fold_in(stream_key, 6), dim), (blocks,), jnp.float32, least / len(shards), top_value / len(shards))
        return jnp.repeat(jnp.exp(heights), shape[dim] // blocks).reshape((-1,) + (1,) * (len(shape) - dim - 1))

    gain = one(*shards[0])
    for cut in shards[1:]:
        gain = gain * one(*cut)
    return gain


def bell_draw(stream_key, shape, deviation, limit, split=(), kind=jnp.bfloat16):
    result = jax.random.normal(stream_key, shape, jnp.float32) * deviation
    if len(split) > 0:
        result = levels(stream_key, shape, split, -0.22, 0.18) * result
    return jnp.clip(result, min=-limit, max=limit).astype(kind)


def setup_inputs(seed: int = 0) -> dict:
    streams_of = jax.random.split(jax.random.key(seed), 8)
    offsets = jnp.clip(10.0 * jax.random.uniform(streams_of[0], (3, NCZ, NCX, NCY, SLOTS), jnp.float32) ** levels(streams_of[0], (3, NCZ, NCX, NCY, SLOTS), ((1, 4), (2, 4), (3, 2)), -0.2, 0.2), 0.0, 10.0)
    type_ids = place_ends(jax.random.randint(streams_of[1], (NCZ, NCX, NCY, SLOTS), 0, NTYPES), jax.random.fold_in(streams_of[1], 1), 0, NTYPES - 1).astype(jnp.int32)
    occupied = draw_occupied(jax.random.fold_in(streams_of[7], 71), 0)
    prior_charges = bell_draw(streams_of[3], (2, NCZ, NCX, NCY, SLOTS), 0.1, 0.6, ((1, 4), (2, 4), (3, 2)), jnp.float32)
    electronegativity = jnp.clip(jax.random.uniform(streams_of[4], (NTYPES,), jnp.float32, 2.0, 10.0), 2.0, 10.0)
    hardness = jnp.clip(jax.random.uniform(streams_of[5], (NTYPES,), jnp.float32, 4.0, 12.0), 4.0, 12.0)
    shielding = jnp.clip(jax.random.uniform(streams_of[6], (NTYPES,), jnp.float32, 0.5, 1.2), 0.5, 1.2)
    return {"offsets": offsets, "type_ids": type_ids, "occupied": occupied, "prior_charges": prior_charges, "electronegativity": electronegativity, "hardness": hardness, "shielding": shielding}


coulomb_factor = 14.4
cell_edge = 10.0

def per_atom(values_table, type_ids):
    summed = jnp.zeros(type_ids.shape, jnp.float32)
    for species in range(values_table.shape[0]):
        summed = summed + jnp.where(type_ids == species, values_table[species], 0.0)
    return summed

def pair_sum(local_geo, beside, remote, shift):
    delta_z = shift[0] * cell_edge + beside[0][..., None, :] - local_geo[0][..., :, None]
    delta_x = shift[1] * cell_edge + beside[1][..., None, :] - local_geo[1][..., :, None]
    delta_y = shift[2] * cell_edge + beside[2][..., None, :] - local_geo[2][..., :, None]
    squared = delta_z * delta_z + delta_x * delta_x + delta_y * delta_y
    fraction = jnp.sqrt(squared) / cell_edge
    reach = jnp.maximum(1.0 - fraction, 0.0)
    reach = reach * reach
    taper = reach * reach * (4.0 * fraction + 1.0)
    kernel = coulomb_factor * lax.rsqrt(squared + local_geo[3][..., :, None] + beside[3][..., None, :]) * taper
    return lax.optimization_barrier(jnp.sum(kernel[None] * remote[..., None, :], axis=-1))

def couple(geometry, field):
    geo_padded = jnp.pad(geometry, ((0, 0), (1, 1), (0, 0), (0, 0), (0, 0)))
    field_padded = jnp.pad(field, ((0, 0), (1, 1), (0, 0), (0, 0), (0, 0)))

    def z_plane(index_z):
        geo_slab = lax.dynamic_slice_in_dim(geo_padded, index_z, 3, 1)
        field_slab = lax.dynamic_slice_in_dim(field_padded, index_z, 3, 1)
        local_geo = geo_slab[:, 1]
        summed = jnp.zeros((field.shape[0],) + local_geo.shape[1:], jnp.float32)
        for off_z in range(3):
            for off_x in range(3):
                for off_y in range(3):
                    beside = jnp.roll(geo_slab[:, off_z], (1 - off_x, 1 - off_y), axis=(1, 2))
                    remote = jnp.roll(field_slab[:, off_z], (1 - off_x, 1 - off_y), axis=(1, 2))
                    summed = summed + pair_sum(local_geo, beside, remote, (off_z - 1, off_x - 1, off_y - 1))
        return summed
    planes = lax.map(z_plane, jnp.arange(NCZ, dtype=jnp.int32))
    return jnp.moveaxis(planes, 0, 1)

def inner_sum(left, right):
    return lax.optimization_barrier(jnp.sum(left * right, axis=(1, 2, 3, 4)))

def expand(scalars):
    return scalars[:, None, None, None, None]

def reference(offsets, type_ids, occupied, prior_charges, electronegativity, hardness, shielding):
    occupancy = occupied.astype(jnp.float32)
    stiffness = per_atom(hardness, type_ids)
    affinity = per_atom(electronegativity, type_ids)
    radius = per_atom(shielding, type_ids)
    geometry = jnp.concatenate([offsets, (radius * radius)[None]], axis=0)

    def operate(field):
        return occupancy[None] * (stiffness[None] * field + couple(geometry, field))
    rhs = jnp.stack([-affinity * occupancy, -occupancy])
    iterate = prior_charges * occupancy[None]
    residual = rhs - operate(iterate)
    direction = residual
    norm_now = inner_sum(residual, residual)
    for iteration in range(ITERS):
        image = operate(direction)
        step_size = norm_now / inner_sum(direction, image)
        iterate = iterate + expand(step_size) * direction
        residual = residual - expand(step_size) * image
        norm_next = inner_sum(residual, residual)
        direction = residual + expand(norm_next / norm_now) * direction
        norm_now = norm_next
    totals = lax.optimization_barrier(jnp.sum(iterate, axis=(1, 2, 3, 4)))
    charges = iterate[0] - totals[0] / totals[1] * iterate[1]
    return (charges, residual)
```

```python
import functools

import jax
import jax.numpy as jnp
from jax import lax
from jax.experimental import pallas as pl
from jax.experimental.pallas import tpu as pltpu
from jax.sharding import PartitionSpec as P

ITERS = 4
AXES = ("gz", "gx", "gy")
MESH = pl.DeviceIdType.MESH

coulomb_factor = 14.4
cell_edge = 10.0
CHUNK = 64
EDGE = (4.0 * coulomb_factor / cell_edge) ** 0.25
SCALE = EDGE / cell_edge
DEPTH = 64


def kernel(
    sizes, dys,
    offsets_in, type_ids_in, occupied_in, prior_in, electro_in, hardness_in, shielding_in,
    charges, residuals,
    offsets, type_ids, occupied, prior, electro, hardness, shielding,
    first, fields, first_edge, edges, pair, left, right, sums, image, parts, mine,
    in_sem, send_sem, recv_sem, part_send, part_recv,
):
    loads = [
        pltpu.make_async_copy(source, target, in_sem.at[k])
        for k, (source, target) in enumerate(
            zip(
                (offsets_in, type_ids_in, occupied_in, prior_in,
                 electro_in, hardness_in, shielding_in),
                (offsets, type_ids, occupied, prior, electro, hardness, shielding),
            )
        )
    ]
    for load in loads:
        load.start()
    nz, nx, ny = sizes
    cells_x, cells_y, slots = type_ids.shape[1:]
    rows = 2 * cells_y
    geo_rows = 4 * cells_y
    cells = cells_x * cells_y
    devices = nz * nx * ny
    sides = len(dys) - 1
    me_z, me_x, me_y = (lax.axis_index(name) for name in AXES)

    at_x = [lax.rem(me_x + d, nx) for d in range(nx)]
    at_y = [lax.rem(me_y + d, ny) for d in range(ny)]

    def each_peer(action):
        def layer(dz, skip):
            z = lax.rem(me_z + dz, nz)
            for dx in range(nx):
                for dy in range(ny):
                    if not (skip and dx == 0 and dy == 0):
                        action((z, at_x[dx], at_y[dy]), (dz * nx + dx) * ny + dy - 1)

        layer(0, True)
        if nz <= 4:
            for dz in range(1, nz):
                layer(dz, False)
        else:
            pl.loop(1, nz)(lambda dz: layer(dz, False))

    barrier = pltpu.get_barrier_semaphore()
    each_peer(
        lambda peer, slot: pl.semaphore_signal(
            barrier, inc=1, device_id=peer, device_id_type=MESH
        )
    )

    def per_atom(table, ids):
        summed = jnp.zeros(ids.shape, jnp.float32)
        for species in range(table.shape[0]):
            summed = summed + jnp.where(ids == species, table[species], 0.0)
        return summed

    for load in loads:
        load.wait()
    occ, stiff, rhs, x = [], [], [], []

    def ends(values):
        return [values[:1], values[cells_y - 1 : cells_y]]

    for i in range(cells_x):
        ids = type_ids[0, i]
        occ_i = occupied[0, i].astype(jnp.float32)
        radius = per_atom(shielding, ids) * SCALE
        geo = [offsets[c, 0, i] * SCALE for c in range(3)] + [radius * radius]
        first[1, i + 1, :geo_rows] = jnp.concatenate(geo, axis=0)
        stiff_i = per_atom(hardness, ids)
        affinity = per_atom(electro, ids)
        occ.append(jnp.concatenate([occ_i, occ_i], axis=0))
        stiff.append(jnp.concatenate([stiff_i, stiff_i], axis=0))
        rhs.append(jnp.concatenate([-affinity * occ_i, -occ_i], axis=0))
        start = jnp.concatenate([prior[0, 0, i] * occ_i, prior[1, 0, i] * occ_i], axis=0)
        x.append(start)
        first[1, i + 1, geo_rows : geo_rows + rows] = start
        pieces = geo + [start[:cells_y], start[cells_y:]]
        first_edge[i] = jnp.concatenate([end for v in pieces for end in ends(v)], axis=0)

    for edge, slot in ((0, 0), (nz - 1, 2)):

        @pl.when(me_z == edge)
        def _():
            first[slot] = jnp.zeros(first.shape[1:], jnp.float32)
            for k in range(ITERS):
                fields[k, slot] = jnp.zeros(fields.shape[2:], jnp.float32)

    messages = [
        (dz, dx, dy)
        for dx_set, dy_set in (((1, -1), dys[1:]), ((1, -1), (0,)), ((0,), dys[1:]), ((0,), (0,)))
        for dz in (1, -1, 0)
        for dx in dx_set
        for dy in dy_set
        if (dz, dx, dy) != (0, 0, 0)
    ]
    turn_x = {d: lax.rem(me_x + d + nx, nx) for d in (0, 1, -1)}
    turn_y = {d: lax.rem(me_y + d + ny, ny) for d in (0, 1, -1)}

    def each_message(stage, buffer, edge, own_rows, name):
        edge_rows = edge.shape[1]
        for dz, dx, dy in messages:
            source, target, count = {
                0: (0, 1, cells_x),
                1: (cells_x - 1, 0, 1),
                -1: (0, cells_x + 1, 1),
            }[dx]
            if dy == 0:
                src = buffer.at[1, pl.ds(source + 1, count), pl.ds(0, own_rows)]
                span = pl.ds(0, own_rows)
            else:
                src = edge.at[pl.ds(source, count)]
                span = pl.ds(own_rows + (dys.index(dy) - 1) * edge_rows, edge_rows)
            at = (stage, 1 - dz, 1 - dx, dys.index(dy))
            copy = pltpu.make_async_remote_copy(
                src_ref=src,
                dst_ref=buffer.at[1 - dz, pl.ds(target, count), span],
                send_sem=send_sem.at[at],
                recv_sem=recv_sem.at[at],
                device_id=(me_z + dz, turn_x[dx], turn_y[dy]),
                device_id_type=MESH,
            )
            act = getattr(copy, name)
            if dz == 0:
                act()
            else:
                other = me_z + dz
                pl.when((other >= 0) & (other < nz))(act)

    def send(*what):
        each_message(*what, "start")

    def sent(*what):
        each_message(*what, "wait_send")

    def receive(what, plane, side, across):
        stage, buffer, edge, own_rows = what
        edge_rows = edge.shape[1]
        count = cells_x if isinstance(side, int) and side == 1 else 1
        for d in range(len(dys)):
            if (d == 0) == across:
                continue
            rows_in = edge_rows if across else own_rows
            landed = buffer.at[1, pl.ds(1, count), pl.ds(0, rows_in)]
            pltpu.make_async_copy(landed, landed, recv_sem.at[stage, plane, side, d]).wait()

    even = lax.rem(me_z, 2) == 0
    near = jnp.where(even, 2, 0)
    far = 2 - near
    has_far = (me_z + far >= 1) & (me_z + far <= nz)
    has_near = (me_z + near >= 1) & (me_z + near <= nz)
    early = jnp.where(me_x == nx - 1, 0, 2)

    def receive_planes(what, planes, side, across):
        for plane in planes:
            if isinstance(plane, int):
                receive(what, plane, side, across)
            else:
                there = has_near if plane is near else has_far
                pl.when(there)(lambda plane=plane: receive(what, plane, side, across))

    opening = (0, first, first_edge, geo_rows + rows)
    pl.semaphore_wait(barrier, devices - 1)
    send(*opening)

    shape = (slots, slots)
    eye = lax.broadcasted_iota(jnp.int32, shape, 0) == lax.broadcasted_iota(jnp.int32, shape, 1)

    def row_at(q, y, base, own_rows, edge_base, edge_rows):
        if y < 0:
            return own_rows + edge_base + 2 * q + 1
        if y >= cells_y:
            return own_rows + (sides - 1) * edge_rows + edge_base + 2 * q
        return base + q * cells_y + y

    geo_rule = (0, geo_rows + rows, 0, 12)
    start_rule = (geo_rows, geo_rows + rows, 8, 12)
    field_rule = (0, rows, 0, 4)

    def inside(i):
        return [1, 2 - 2 * i] if cells_x == 2 else [1]

    def in_block(j, k):
        return 0 <= j + k - 1 < cells_y

    group = lax.broadcasted_iota(jnp.int32, (8, slots), 0)
    role = lax.rem(group, 4)
    lower = group < 4
    ones = jnp.where(group < 3, 1.0, 0.0)
    nought = jnp.zeros((8, slots), jnp.float32)

    def split(values):
        pieces = []
        for _ in range(3):
            piece = values.astype(jnp.bfloat16).astype(jnp.float32)
            pieces.append(piece)
            values = values - piece
        return pieces

    def place(dz, dx, y):
        start = row_at(0, y, *geo_rule)
        step = cells_y if 0 <= y < cells_y else 2
        four = first[dz, dx, pl.ds(start, 4, stride=step), :]
        both = jnp.concatenate([four, four], axis=0)
        centre_z = (jnp.asarray(dz, jnp.int32).astype(jnp.float32) - 1.5) * EDGE
        centre_x = (jnp.asarray(dx, jnp.int32).astype(jnp.float32) - (1.0 + cells_x / 2)) * EDGE
        centre_y = (y - cells_y / 2) * EDGE
        moved = both + jnp.where(
            role == 0, centre_z, jnp.where(role == 1, centre_x, jnp.where(role == 2, centre_y, 0.0))
        )
        squares = jnp.where((role == 3) | (group > 3), 0.0, moved * moved)
        return moved, jnp.sum(squares, axis=0, keepdims=True), four[3:4]

    def slot_at(dz, dx, y):
        return (dz * (cells_x + 2) + dx) * (cells_y + 2) + y + 1

    def offer(dz, dx, y):
        moved, length, spread = place(dz, dx, y)
        last = jnp.where(lower, length, length + spread)
        p1, p2, p3 = split(jnp.where(role == 3, last, moved))
        to = slot_at(dz, dx, y)
        for half in range(2):
            kept = [
                jnp.where(lower, p, 0.0) if half == 0 else jnp.where(lower, 0.0, p)
                for p in (p1, p2, p3)
            ]
            lines = [kept[q] for q in (0, 1, 2, 0, 1, 0)] + [ones, ones if half else nought]
            right[to, :, half * slots : (half + 1) * slots] = jnp.concatenate(
                lines, axis=0
            ).astype(jnp.bfloat16)

    def take(i, j):
        moved, length, spread = place(1, i + 1, j)
        a1, a2, a3 = split(-2.0 * moved)

        def stacked(value):
            v1, v2, v3 = split(value)
            return jnp.where(group == 0, v1, jnp.where(group == 1, v2, jnp.where(group == 2, v3, 0.0)))

        one = jnp.where(role == 3, 1.0, a1)
        two = jnp.where(role == 3, 0.0, a2)
        three = jnp.where(role == 3, 0.0, a3)
        lines = [one, one, one, two, two, three, stacked(length), stacked(spread)]
        left[i * cells_y + j] = jnp.concatenate(lines, axis=0).T.astype(jnp.bfloat16)

    def couple(i, j, dz, dx, k):
        cell = i * cells_y + j
        other = right[slot_at(dz, i + dx, j + k - 1)]
        for part in range(slots // CHUNK):
            span = pl.ds(part * CHUNK, CHUNK)
            both = jnp.dot(left[cell, span], other, preferred_element_type=jnp.float32)
            squared = jnp.maximum(both[:, :slots], 1e-30)
            apart = squared * lax.rsqrt(squared)
            reach = jnp.maximum(EDGE - apart, 0.0)
            reach = reach * reach
            pair[cell, (dz * 3 + dx) * 3 + k, span] = (
                reach * reach * (apart + EDGE / 4) * lax.rsqrt(both[:, slots:])
            )

    ends_y = sorted({0, cells_y - 1})

    def build(what):
        def plane(dz):
            @pl.loop(0, cells_x)
            def _(i):
                for y in range(cells_y):
                    offer(dz, i + 1, y)

            @pl.loop(0, cells_x)
            def _(i):
                for j in range(cells_y):
                    for dx in inside(i):
                        for k in range(3):
                            if in_block(j, k):
                                couple(i, j, dz, dx, k)

        @pl.loop(0, cells_x)
        def _(i):
            for j in range(cells_y):
                take(i, j)

        plane(1)
        for dz in (near, far):
            receive_planes(what, (dz,), 1, False)
            plane(dz)
        receive_planes(what, (1, near, far), 1, True)
        for dz in (1, near, far):

            @pl.loop(0, cells_x)
            def _(i):
                for y in (-1, cells_y):
                    offer(dz, i + 1, y)

        @pl.loop(0, cells_x)
        def _(i):
            for dz in (1, near, far):
                for j in ends_y:
                    for dx in inside(i):
                        for k in range(3):
                            if not in_block(j, k):
                                couple(i, j, dz, dx, k)

        @pl.loop(0, 2)
        def _(turn):
            side = jnp.where(turn == 0, early, 2 - early)
            i = (cells_x - 1) * (side // 2)
            receive_planes(what, (1, near, far), side, False)
            for dz in (1, near, far):
                for y in range(cells_y):
                    offer(dz, i + side, y)
            for dz in (1, near, far):
                for j in range(cells_y):
                    for k in range(3):
                        if in_block(j, k):
                            couple(i, j, dz, side, k)
            receive_planes(what, (1, near, far), side, True)
            for dz in (1, near, far):
                for y in (-1, cells_y):
                    offer(dz, i + side, y)
            for dz in (1, near, far):
                for j in ends_y:
                    for k in range(3):
                        if not in_block(j, k):
                            couple(i, j, dz, side, k)

    def add_pairs(buffer, rule, i, j, entries, fresh):
        if fresh:
            total = [jnp.zeros(shape, jnp.float32) for _ in range(2)]
        else:
            total = [sums[i, s * cells_y + j] for s in range(2)]
        for dz, dx, k in entries:
            tile = buffer.at[dz, i + dx]
            block = pair[i * cells_y + j, (dz * 3 + dx) * 3 + k]
            for s in range(2):
                at = row_at(s, j + k - 1, *rule)
                total[s] = total[s] + block * tile[at : at + 1, :]
        for s in range(2):
            sums[i, s * cells_y + j] = total[s]

    def gather(i):
        lines = []
        for row in range(rows):
            column = jnp.sum(sums[i, row], axis=1, keepdims=True)
            lines.append(jnp.sum(jnp.where(eye, column, 0.0), axis=0, keepdims=True))
        image[i] = jnp.concatenate(lines, axis=0)

    def operate(buffer, rule, field, what=None):
        def arrive(*args):
            if what is not None:
                receive_planes(what, *args)

        def plane(dz, fresh):
            @pl.loop(0, cells_x)
            def _(i):
                for j in range(cells_y):
                    add_pairs(
                        buffer, rule, i, j,
                        [(dz, dx, k) for dx in inside(i) for k in range(3) if in_block(j, k)],
                        fresh,
                    )

        every = (1, near, far)
        plane(1, True)
        for dz in (near, far):
            arrive((dz,), 1, False)
            plane(dz, False)
        arrive(every, 1, True)

        @pl.loop(0, cells_x)
        def _(i):
            for j in ends_y:
                add_pairs(
                    buffer, rule, i, j,
                    [
                        (dz, dx, k)
                        for dz in every for dx in inside(i) for k in range(3)
                        if not in_block(j, k)
                    ],
                    False,
                )

        @pl.loop(0, 2)
        def _(turn):
            side = jnp.where(turn == 0, early, 2 - early)
            i = (cells_x - 1) * (side // 2)
            arrive(every, side, False)
            for j in range(cells_y):
                add_pairs(
                    buffer, rule, i, j,
                    [(dz, side, k) for dz in every for k in range(3) if in_block(j, k)],
                    False,
                )
            arrive(every, side, True)
            for j in ends_y:
                add_pairs(
                    buffer, rule, i, j,
                    [(dz, side, k) for dz in every for k in range(3) if not in_block(j, k)],
                    False,
                )
            gather(i)

        return [occ[i] * (stiff[i] * field[i] + image[i]) for i in range(cells_x)]

    tile_shape = (rows, slots)
    lane = lax.broadcasted_iota(jnp.int32, tile_shape, 1)
    second = lax.broadcasted_iota(jnp.int32, tile_shape, 0) >= cells_y
    slot_of = lane - jnp.where(second, 8, 0)

    def part_copy(stage, peer, slot):
        return pltpu.make_async_remote_copy(
            src_ref=mine.at[stage],
            dst_ref=parts.at[stage, slot],
            send_sem=part_send.at[stage],
            recv_sem=part_recv.at[stage],
            device_id=peer,
            device_id_type=MESH,
        )

    def start_sums(stage, quantities):
        packed = jnp.zeros(tile_shape, jnp.float32)
        for k, quantity in enumerate(quantities):
            column = jnp.sum(functools.reduce(jnp.add, quantity), axis=1, keepdims=True)
            packed = jnp.where(slot_of == k, column, packed)
        mine[stage] = jnp.sum(packed, axis=0, keepdims=True)
        each_peer(lambda peer, slot: part_copy(stage, peer, slot).start())

    def finish_sums(stage, count):
        everything = parts.at[stage]
        pltpu.make_async_copy(everything, everything, part_recv.at[stage]).wait()
        row = mine[stage] + jnp.sum(parts[stage], axis=0)
        pltpu.make_async_copy(everything, everything, part_send.at[stage]).wait()
        return [
            jnp.where(
                second,
                jnp.broadcast_to(row[:, 8 + k : 9 + k], tile_shape),
                jnp.broadcast_to(row[:, k : k + 1], tile_shape),
            )
            for k in range(count)
        ]

    span = range(cells_x)

    def exchange_and_operate(stage, field, meanwhile=None):
        buffer, edge = fields.at[stage - 1], edges.at[stage - 1]
        for i in span:
            buffer[1, i + 1, :rows] = field[i]
            pieces = [field[i][:cells_y], field[i][cells_y:]]
            edge[i] = jnp.concatenate([end for v in pieces for end in ends(v)], axis=0)
        what = (stage, buffer, edge, rows)
        send(*what)
        if meanwhile is not None:
            meanwhile()
        out = operate(buffer, field_rule, field, what)
        sent(*what)
        return out

    build(opening)
    started = operate(first, start_rule, x)
    sent(*opening)
    r = [rhs[i] - started[i] for i in span]
    w = exchange_and_operate(1, r)

    p = s = z = None
    for stage in range(ITERS):
        quantities = [[r[i] * r[i] for i in span], [w[i] * r[i] for i in span]]
        last = stage == ITERS - 1
        if last:
            quantities += [x, r, p]
        go = functools.partial(start_sums, stage, quantities)
        n = go() if last else exchange_and_operate(stage + 2, w, go)
        found = finish_sums(stage, len(quantities))
        gamma, delta = found[:2]
        if stage == 0:
            beta = None
            alpha = gamma / delta
            p, s, z = r, w, n
        else:
            beta = gamma / gamma_before
            alpha = gamma / (delta - beta * gamma / alpha)
            p = [r[i] + beta * p[i] for i in span]
            s = [w[i] + beta * s[i] for i in span]
            if not last:
                z = [n[i] + beta * z[i] for i in span]
        gamma_before = gamma
        x = [x[i] + alpha * p[i] for i in span]
        r = [r[i] - alpha * s[i] for i in span]
        if not last:
            w = [w[i] - alpha * z[i] for i in span]
    totals = found[2] + alpha * (found[3] + beta * found[4])
    ratio = totals[:cells_y] / totals[cells_y:]
    for i in span:
        charges[0, i] = x[i][:cells_y] - ratio * x[i][cells_y:]
        residuals[0, 0, i] = r[i][:cells_y]
        residuals[1, 0, i] = r[i][cells_y:]


def per_device(sizes, *arrays):
    type_ids = arrays[1]
    cells_x, cells_y, slots = type_ids.shape[1:]
    cells = cells_x * cells_y
    rows = 2 * cells_y
    devices = sizes[0] * sizes[1] * sizes[2]
    dys = (0, 1) if sizes[2] == 2 else (0, 1, -1)
    halo = (3, cells_x + 2)
    sides = len(dys) - 1
    vmem = pl.BlockSpec(memory_space=pltpu.VMEM)
    return pl.pallas_call(
        functools.partial(kernel, sizes, dys),
        out_shape=(
            pltpu.VMEM(type_ids.shape, jnp.float32),
            pltpu.VMEM((2,) + type_ids.shape, jnp.float32),
        ),
        in_specs=[pl.BlockSpec(memory_space=pl.ANY)] * 7,
        out_specs=(vmem, vmem),
        scratch_shapes=[
            *(pltpu.VMEM(array.shape, array.dtype) for array in arrays[:4]),
            *(pltpu.SMEM(array.shape, array.dtype) for array in arrays[4:]),
            pltpu.VMEM(halo + (6 * cells_y + 12 * sides, slots), jnp.float32),
            pltpu.VMEM((ITERS,) + halo + (rows + 4 * sides, slots), jnp.float32),
            pltpu.VMEM((cells_x, 12, slots), jnp.float32),
            pltpu.VMEM((ITERS, cells_x, 4, slots), jnp.float32),
            pltpu.VMEM((cells, 27, slots, slots), jnp.float32),
            pltpu.VMEM((cells, slots, DEPTH), jnp.bfloat16),
            pltpu.VMEM((halo[0] * halo[1] * (cells_y + 2), DEPTH, 2 * slots), jnp.bfloat16),
            pltpu.VMEM((cells_x, rows, slots, slots), jnp.float32),
            pltpu.VMEM((cells_x, rows, slots), jnp.float32),
            pltpu.VMEM((ITERS, devices - 1, 1, slots), jnp.float32),
            pltpu.VMEM((ITERS, 1, slots), jnp.float32),
            pltpu.SemaphoreType.DMA((len(arrays),)),
            pltpu.SemaphoreType.DMA((ITERS + 1, 3, 3, len(dys))),
            pltpu.SemaphoreType.DMA((ITERS + 1, 3, 3, len(dys))),
            pltpu.SemaphoreType.DMA((ITERS,)),
            pltpu.SemaphoreType.DMA((ITERS,)),
        ],
        compiler_params=pltpu.CompilerParams(
            collective_id=0, has_side_effects=True, vmem_limit_bytes=60 * 1024 * 1024
        ),
    )(*arrays)


def solution(mesh):
    sizes = tuple(mesh.shape[name] for name in AXES)
    in_specs = (
        P(None, "gz", "gx", "gy", None),
        P("gz", "gx", "gy", None),
        P("gz", "gx", "gy", None),
        P(None, "gz", "gx", "gy", None),
        P(),
        P(),
        P(),
    )
    out_specs = (P("gz", "gx", "gy", None), P(None, "gz", "gx", "gy", None))
    return jax.shard_map(
        functools.partial(per_device, sizes),
        mesh=mesh,
        in_specs=in_specs,
        out_specs=out_specs,
        check_vma=False,
    )
```

```python
import functools

import jax
import jax.numpy as jnp
from jax import lax
from jax.experimental import pallas as pl
from jax.experimental.pallas import tpu as pltpu
from jax.sharding import PartitionSpec as P

ITERS = 4
AXES = ("gz", "gx", "gy")
MESH = pl.DeviceIdType.MESH

coulomb_factor = 14.4
cell_edge = 10.0
CHUNK = 64
EDGE = (4.0 * coulomb_factor / cell_edge) ** 0.25
SCALE = EDGE / cell_edge
DEPTH = 64


def kernel(
    sizes, dys,
    offsets_in, type_ids_in, occupied_in, prior_in, electro_in, hardness_in, shielding_in,
    charges, residuals,
    offsets, type_ids, occupied, prior, electro, hardness, shielding,
    first, fields, first_edge, edges, pair, left, right, sums, image, parts, mine,
    in_sem, send_sem, recv_sem, part_send, part_recv,
):
    loads = [
        pltpu.make_async_copy(source, target, in_sem.at[k])
        for k, (source, target) in enumerate(
            zip(
                (offsets_in, type_ids_in, occupied_in, prior_in,
                 electro_in, hardness_in, shielding_in),
                (offsets, type_ids, occupied, prior, electro, hardness, shielding),
            )
        )
    ]
    for load in loads:
        load.start()
    nz, nx, ny = sizes
    cells_x, cells_y, slots = type_ids.shape[1:]
    rows = 2 * cells_y
    geo_rows = 4 * cells_y
    cells = cells_x * cells_y
    devices = nz * nx * ny
    sides = len(dys) - 1
    me_z, me_x, me_y = (lax.axis_index(name) for name in AXES)

    at_x = [lax.rem(me_x + d, nx) for d in range(nx)]
    at_y = [lax.rem(me_y + d, ny) for d in range(ny)]

    def each_peer(action):
        def layer(dz, skip):
            z = lax.rem(me_z + dz, nz)
            for dx in range(nx):
                for dy in range(ny):
                    if not (skip and dx == 0 and dy == 0):
                        action((z, at_x[dx], at_y[dy]), (dz * nx + dx) * ny + dy - 1)

        layer(0, True)
        if nz <= 4:
            for dz in range(1, nz):
                layer(dz, False)
        else:
            pl.loop(1, nz)(lambda dz: layer(dz, False))

    barrier = pltpu.get_barrier_semaphore()
    each_peer(
        lambda peer, slot: pl.semaphore_signal(
            barrier, inc=1, device_id=peer, device_id_type=MESH
        )
    )

    def per_atom(table, ids):
        summed = jnp.zeros(ids.shape, jnp.float32)
        for species in range(table.shape[0]):
            summed = summed + jnp.where(ids == species, table[species], 0.0)
        return summed

    for load in loads:
        load.wait()
    occ, stiff, rhs, x = [], [], [], []

    def ends(values):
        return [values[:1], values[cells_y - 1 : cells_y]]

    for i in range(cells_x):
        ids = type_ids[0, i]
        occ_i = occupied[0, i].astype(jnp.float32)
        radius = per_atom(shielding, ids) * SCALE
        geo = [offsets[c, 0, i] * SCALE for c in range(3)] + [radius * radius]
        first[1, i + 1, :geo_rows] = jnp.concatenate(geo, axis=0)
        stiff_i = per_atom(hardness, ids)
        affinity = per_atom(electro, ids)
        occ.append(jnp.concatenate([occ_i, occ_i], axis=0))
        stiff.append(jnp.concatenate([stiff_i, stiff_i], axis=0))
        rhs.append(jnp.concatenate([-affinity * occ_i, -occ_i], axis=0))
        start = jnp.concatenate([prior[0, 0, i] * occ_i, prior[1, 0, i] * occ_i], axis=0)
        x.append(start)
        first[1, i + 1, geo_rows : geo_rows + rows] = start
        pieces = geo + [start[:cells_y], start[cells_y:]]
        first_edge[i] = jnp.concatenate([end for v in pieces for end in ends(v)], axis=0)

    for edge, slot in ((0, 0), (nz - 1, 2)):

        @pl.when(me_z == edge)
        def _():
            first[slot] = jnp.zeros(first.shape[1:], jnp.float32)
            for k in range(ITERS):
                fields[k, slot] = jnp.zeros(fields.shape[2:], jnp.float32)

    messages = [
        (dz, dx, dy)
        for dx_set, dy_set in (((1, -1), dys[1:]), ((1, -1), (0,)), ((0,), dys[1:]), ((0,), (0,)))
        for dz in (1, -1, 0)
        for dx in dx_set
        for dy in dy_set
        if (dz, dx, dy) != (0, 0, 0)
    ]
    turn_x = {d: lax.rem(me_x + d + nx, nx) for d in (0, 1, -1)}
    turn_y = {d: lax.rem(me_y + d + ny, ny) for d in (0, 1, -1)}

    def each_message(stage, buffer, edge, own_rows, name):
        edge_rows = edge.shape[1]
        for dz, dx, dy in messages:
            source, target, count = {
                0: (0, 1, cells_x),
                1: (cells_x - 1, 0, 1),
                -1: (0, cells_x + 1, 1),
            }[dx]
            if dy == 0:
                src = buffer.at[1, pl.ds(source + 1, count), pl.ds(0, own_rows)]
                span = pl.ds(0, own_rows)
            else:
                src = edge.at[pl.ds(source, count)]
                span = pl.ds(own_rows + (dys.index(dy) - 1) * edge_rows, edge_rows)
            at = (stage, 1 - dz, 1 - dx, dys.index(dy))
            copy = pltpu.make_async_remote_copy(
                src_ref=src,
                dst_ref=buffer.at[1 - dz, pl.ds(target, count), span],
                send_sem=send_sem.at[at],
                recv_sem=recv_sem.at[at],
                device_id=(me_z + dz, turn_x[dx], turn_y[dy]),
                device_id_type=MESH,
            )
            act = getattr(copy, name)
            if dz == 0:
                act()
            else:
                other = me_z + dz
                pl.when((other >= 0) & (other < nz))(act)

    def send(*what):
        each_message(*what, "start")

    def sent(*what):
        each_message(*what, "wait_send")

    def receive(what, plane, side, across):
        stage, buffer, edge, own_rows = what
        edge_rows = edge.shape[1]
        count = cells_x if isinstance(side, int) and side == 1 else 1
        for d in range(len(dys)):
            if (d == 0) == across:
                continue
            rows_in = edge_rows if across else own_rows
            landed = buffer.at[1, pl.ds(1, count), pl.ds(0, rows_in)]
            pltpu.make_async_copy(landed, landed, recv_sem.at[stage, plane, side, d]).wait()

    even = lax.rem(me_z, 2) == 0
    near = jnp.where(even, 2, 0)
    far = 2 - near
    has_far = (me_z + far >= 1) & (me_z + far <= nz)
    has_near = (me_z + near >= 1) & (me_z + near <= nz)
    early = jnp.where(me_x == nx - 1, 0, 2)

    def receive_planes(what, planes, side, across):
        for plane in planes:
            if isinstance(plane, int):
                receive(what, plane, side, across)
            else:
                there = has_near if plane is near else has_far
                pl.when(there)(lambda plane=plane: receive(what, plane, side, across))

    opening = (0, first, first_edge, geo_rows + rows)
    pl.semaphore_wait(barrier, devices - 1)
    send(*opening)

    shape = (slots, slots)
    eye = lax.broadcasted_iota(jnp.int32, shape, 0) == lax.broadcasted_iota(jnp.int32, shape, 1)

    def row_at(q, y, base, own_rows, edge_base, edge_rows):
        if y < 0:
            return own_rows + edge_base + 2 * q + 1
        if y >= cells_y:
            return own_rows + (sides - 1) * edge_rows + edge_base + 2 * q
        return base + q * cells_y + y

    geo_rule = (0, geo_rows + rows, 0, 12)
    start_rule = (geo_rows, geo_rows + rows, 8, 12)
    field_rule = (0, rows, 0, 4)

    def inside(i):
        return [1, 2 - 2 * i] if cells_x == 2 else [1]

    def in_block(j, k):
        return 0 <= j + k - 1 < cells_y

    group = lax.broadcasted_iota(jnp.int32, (8, slots), 0)
    role = lax.rem(group, 4)
    lower = group < 4
    ones = jnp.where(group < 3, 1.0, 0.0)
    nought = jnp.zeros((8, slots), jnp.float32)

    def split(values):
        pieces = []
        for _ in range(3):
            piece = values.astype(jnp.bfloat16).astype(jnp.float32)
            pieces.append(piece)
            values = values - piece
        return pieces

    def place(dz, dx, y):
        start = row_at(0, y, *geo_rule)
        step = cells_y if 0 <= y < cells_y else 2
        four = first[dz, dx, pl.ds(start, 4, stride=step), :]
        both = jnp.concatenate([four, four], axis=0)
        centre_z = (jnp.asarray(dz, jnp.int32).astype(jnp.float32) - 1.5) * EDGE
        centre_x = (jnp.asarray(dx, jnp.int32).astype(jnp.float32) - (1.0 + cells_x / 2)) * EDGE
        centre_y = (y - cells_y / 2) * EDGE
        moved = both + jnp.where(
            role == 0, centre_z, jnp.where(role == 1, centre_x, jnp.where(role == 2, centre_y, 0.0))
        )
        squares = jnp.where((role == 3) | (group > 3), 0.0, moved * moved)
        return moved, jnp.sum(squares, axis=0, keepdims=True), four[3:4]

    def slot_at(dz, dx, y):
        return (dz * (cells_x + 2) + dx) * (cells_y + 2) + y + 1

    def offer(dz, dx, y):
        moved, length, spread = place(dz, dx, y)
        last = jnp.where(lower, length, length + spread)
        p1, p2, p3 = split(jnp.where(role == 3, last, moved))
        to = slot_at(dz, dx, y)
        for half in range(2):
            kept = [
                jnp.where(lower, p, 0.0) if half == 0 else jnp.where(lower, 0.0, p)
                for p in (p1, p2, p3)
            ]
            lines = [kept[q] for q in (0, 1, 2, 0, 1, 0)] + [ones, ones if half else nought]
            right[to, :, half * slots : (half + 1) * slots] = jnp.concatenate(
                lines, axis=0
            ).astype(jnp.bfloat16)

    def take(i, j):
        moved, length, spread = place(1, i + 1, j)
        a1, a2, a3 = split(-2.0 * moved)

        def stacked(value):
            v1, v2, v3 = split(value)
            return jnp.where(group == 0, v1, jnp.where(group == 1, v2, jnp.where(group == 2, v3, 0.0)))

        one = jnp.where(role == 3, 1.0, a1)
        two = jnp.where(role == 3, 0.0, a2)
        three = jnp.where(role == 3, 0.0, a3)
        lines = [one, one, one, two, two, three, stacked(length), stacked(spread)]
        left[i * cells_y + j] = jnp.concatenate(lines, axis=0).T.astype(jnp.bfloat16)

    def couple(i, j, dz, dx, k):
        cell = i * cells_y + j
        other = right[slot_at(dz, i + dx, j + k - 1)]
        for part in range(slots // CHUNK):
            span = pl.ds(part * CHUNK, CHUNK)
            both = jnp.dot(left[cell, span], other, preferred_element_type=jnp.float32)
            squared = jnp.clip(both[:, :slots], 1e-30, EDGE * EDGE)
            apart = squared * lax.rsqrt(squared)
            reach = EDGE - apart
            reach = reach * reach
            pair[cell, (dz * 3 + dx) * 3 + k, span] = (
                reach * reach * (apart + EDGE / 4) * lax.rsqrt(both[:, slots:])
            )

    ends_y = sorted({0, cells_y - 1})

    every = (1, near, far)
    inner, outer = range(cells_y), (-1, cells_y)

    def build(what):
        def plane(dz):
            @pl.loop(0, cells_x)
            def _(i):
                for y in inner:
                    offer(dz, i + 1, y)

            for i in range(cells_x):
                for j in range(cells_y):
                    for dx in inside(i):
                        for k in range(3):
                            if in_block(j, k):
                                couple(i, j, dz, dx, k)

        @pl.loop(0, cells_x)
        def _(i):
            for j in range(cells_y):
                take(i, j)

        plane(1)
        for dz in (near, far):
            receive_planes(what, (dz,), 1, False)
            plane(dz)
        receive_planes(what, every, 1, True)
        for dz in every:

            @pl.loop(0, cells_x)
            def _(i):
                for y in outer:
                    offer(dz, i + 1, y)

        for i in range(cells_x):
            for dz in every:
                for j in ends_y:
                    for dx in inside(i):
                        for k in range(3):
                            if not in_block(j, k):
                                couple(i, j, dz, dx, k)

    def side_of(turn):
        side = early if turn == 0 else 2 - early
        return side, (cells_x - 1) * (side // 2)

    def accept(what, side, i):
        receive_planes(what, every, side, False)
        receive_planes(what, every, side, True)
        for dz in every:
            for y in (*inner, *outer):
                offer(dz, i + side, y)

    def couple_side(side, i):
        for dz in every:
            for j in range(cells_y):
                for k in range(3):
                    couple(i, j, dz, side, k)

    def add_pairs(buffer, rule, i, j, entries, fresh):
        if fresh:
            total = [jnp.zeros(shape, jnp.float32) for _ in range(2)]
        else:
            total = [sums[i, s * cells_y + j] for s in range(2)]
        for dz, dx, k in entries:
            tile = buffer.at[dz, i + dx]
            block = pair[i * cells_y + j, (dz * 3 + dx) * 3 + k]
            for s in range(2):
                at = row_at(s, j + k - 1, *rule)
                total[s] = total[s] + block * tile[at : at + 1, :]
        for s in range(2):
            sums[i, s * cells_y + j] = total[s]

    def gather(i):
        lines = []
        for row in range(rows):
            column = jnp.sum(sums[i, row], axis=1, keepdims=True)
            lines.append(jnp.sum(jnp.where(eye, column, 0.0), axis=0, keepdims=True))
        image[i] = jnp.concatenate(lines, axis=0)

    def update(field):
        return [occ[i] * (stiff[i] * field[i] + image[i]) for i in range(cells_x)]

    def plane_pairs(dz, i, j):
        return [(dz, dx, k) for dx in inside(i) for k in range(3) if in_block(j, k)]

    def end_pairs(i, j):
        return [
            (dz, dx, k)
            for dz in every for dx in inside(i) for k in range(3)
            if not in_block(j, k)
        ]

    def first_image(what, field):
        buffer, rule = what[1], start_rule

        @pl.loop(0, cells_x)
        def _(i):
            for j in range(cells_y):
                pairs = [p for dz in every for p in plane_pairs(dz, i, j)] + end_pairs(i, j)
                add_pairs(buffer, rule, i, j, pairs, True)

        sides = [side_of(turn) for turn in range(2)]
        for side, i in sides:
            accept(what, side, i)
            couple_side(side, i)

        @pl.loop(0, cells_x)
        def _(i):
            side = 2 * i
            for j in range(cells_y):
                pairs = [(dz, side, k) for dz in every for k in range(3)]
                add_pairs(buffer, rule, i, j, pairs, False)
            gather(i)

        return update(field)

    def operate(buffer, rule, field, what):
        def plane(dz, fresh):
            @pl.loop(0, cells_x)
            def _(i):
                for j in range(cells_y):
                    add_pairs(buffer, rule, i, j, plane_pairs(dz, i, j), fresh)

        plane(1, True)
        for dz in (near, far):
            receive_planes(what, (dz,), 1, False)
            plane(dz, False)
        receive_planes(what, every, 1, True)

        @pl.loop(0, cells_x)
        def _(i):
            for j in ends_y:
                add_pairs(buffer, rule, i, j, end_pairs(i, j), False)

        @pl.loop(0, 2)
        def _(turn):
            side = jnp.where(turn == 0, early, 2 - early)
            i = (cells_x - 1) * (side // 2)
            for within in (True, False):
                receive_planes(what, every, side, not within)
                for j in range(cells_y) if within else ends_y:
                    pairs = [(dz, side, k) for dz in every for k in range(3) if in_block(j, k) == within]
                    add_pairs(buffer, rule, i, j, pairs, False)
            gather(i)

        return update(field)

    tile_shape = (rows, slots)
    lane = lax.broadcasted_iota(jnp.int32, tile_shape, 1)
    second = lax.broadcasted_iota(jnp.int32, tile_shape, 0) >= cells_y
    slot_of = lane - jnp.where(second, 8, 0)

    def part_copy(stage, peer, slot):
        return pltpu.make_async_remote_copy(
            src_ref=mine.at[stage],
            dst_ref=parts.at[stage, slot],
            send_sem=part_send.at[stage],
            recv_sem=part_recv.at[stage],
            device_id=peer,
            device_id_type=MESH,
        )

    def start_sums(stage, quantities):
        packed = jnp.zeros(tile_shape, jnp.float32)
        for k, quantity in enumerate(quantities):
            column = jnp.sum(functools.reduce(jnp.add, quantity), axis=1, keepdims=True)
            packed = jnp.where(slot_of == k, column, packed)
        mine[stage] = jnp.sum(packed, axis=0, keepdims=True)
        each_peer(lambda peer, slot: part_copy(stage, peer, slot).start())

    def finish_sums(stage, count):
        everything = parts.at[stage]
        pltpu.make_async_copy(everything, everything, part_recv.at[stage]).wait()
        row = mine[stage] + jnp.sum(parts[stage], axis=0)
        pltpu.make_async_copy(everything, everything, part_send.at[stage]).wait()
        return [
            jnp.where(
                second,
                jnp.broadcast_to(row[:, 8 + k : 9 + k], tile_shape),
                jnp.broadcast_to(row[:, k : k + 1], tile_shape),
            )
            for k in range(count)
        ]

    span = range(cells_x)

    def exchange_and_operate(stage, field, meanwhile=None):
        buffer, edge = fields.at[stage - 1], edges.at[stage - 1]
        for i in span:
            buffer[1, i + 1, :rows] = field[i]
            pieces = [field[i][:cells_y], field[i][cells_y:]]
            edge[i] = jnp.concatenate([end for v in pieces for end in ends(v)], axis=0)
        what = (stage, buffer, edge, rows)
        send(*what)
        if meanwhile is not None:
            meanwhile()
        out = operate(buffer, field_rule, field, what)
        sent(*what)
        return out

    build(opening)
    started = first_image(opening, x)
    sent(*opening)
    r = [rhs[i] - started[i] for i in span]
    w = exchange_and_operate(1, r)

    p = s = z = None
    for stage in range(ITERS):
        quantities = [[r[i] * r[i] for i in span], [w[i] * r[i] for i in span]]
        last = stage == ITERS - 1
        if last:
            quantities += [x, r, p]
        go = functools.partial(start_sums, stage, quantities)
        n = go() if last else exchange_and_operate(stage + 2, w, go)
        found = finish_sums(stage, len(quantities))
        gamma, delta = found[:2]
        if stage == 0:
            beta = None
            alpha = gamma / delta
            p, s, z = r, w, n
        else:
            beta = gamma / gamma_before
            alpha = gamma / (delta - beta * gamma / alpha)
            p = [r[i] + beta * p[i] for i in span]
            s = [w[i] + beta * s[i] for i in span]
            if not last:
                z = [n[i] + beta * z[i] for i in span]
        gamma_before = gamma
        x = [x[i] + alpha * p[i] for i in span]
        r = [r[i] - alpha * s[i] for i in span]
        if not last:
            w = [w[i] - alpha * z[i] for i in span]
    totals = found[2] + alpha * (found[3] + beta * found[4])
    ratio = totals[:cells_y] / totals[cells_y:]
    for i in span:
        charges[0, i] = x[i][:cells_y] - ratio * x[i][cells_y:]
        residuals[0, 0, i] = r[i][:cells_y]
        residuals[1, 0, i] = r[i][cells_y:]


def per_device(sizes, *arrays):
    type_ids = arrays[1]
    cells_x, cells_y, slots = type_ids.shape[1:]
    cells = cells_x * cells_y
    rows = 2 * cells_y
    devices = sizes[0] * sizes[1] * sizes[2]
    dys = (0, 1) if sizes[2] == 2 else (0, 1, -1)
    halo = (3, cells_x + 2)
    sides = len(dys) - 1
    vmem = pl.BlockSpec(memory_space=pltpu.VMEM)
    return pl.pallas_call(
        functools.partial(kernel, sizes, dys),
        out_shape=(
            pltpu.VMEM(type_ids.shape, jnp.float32),
            pltpu.VMEM((2,) + type_ids.shape, jnp.float32),
        ),
        in_specs=[pl.BlockSpec(memory_space=pl.ANY)] * 7,
        out_specs=(vmem, vmem),
        scratch_shapes=[
            *(pltpu.VMEM(array.shape, array.dtype) for array in arrays[:4]),
            *(pltpu.SMEM(array.shape, array.dtype) for array in arrays[4:]),
            pltpu.VMEM(halo + (6 * cells_y + 12 * sides, slots), jnp.float32),
            pltpu.VMEM((ITERS,) + halo + (rows + 4 * sides, slots), jnp.float32),
            pltpu.VMEM((cells_x, 12, slots), jnp.float32),
            pltpu.VMEM((ITERS, cells_x, 4, slots), jnp.float32),
            pltpu.VMEM((cells, 27, slots, slots), jnp.float32),
            pltpu.VMEM((cells, slots, DEPTH), jnp.bfloat16),
            pltpu.VMEM((halo[0] * halo[1] * (cells_y + 2), DEPTH, 2 * slots), jnp.bfloat16),
            pltpu.VMEM((cells_x, rows, slots, slots), jnp.float32),
            pltpu.VMEM((cells_x, rows, slots), jnp.float32),
            pltpu.VMEM((ITERS, devices - 1, 1, slots), jnp.float32),
            pltpu.VMEM((ITERS, 1, slots), jnp.float32),
            pltpu.SemaphoreType.DMA((len(arrays),)),
            pltpu.SemaphoreType.DMA((ITERS + 1, 3, 3, len(dys))),
            pltpu.SemaphoreType.DMA((ITERS + 1, 3, 3, len(dys))),
            pltpu.SemaphoreType.DMA((ITERS,)),
            pltpu.SemaphoreType.DMA((ITERS,)),
        ],
        compiler_params=pltpu.CompilerParams(
            collective_id=0, has_side_effects=True, vmem_limit_bytes=60 * 1024 * 1024
        ),
    )(*arrays)


def solution(mesh):
    sizes = tuple(mesh.shape[name] for name in AXES)
    in_specs = (
        P(None, "gz", "gx", "gy", None),
        P("gz", "gx", "gy", None),
        P("gz", "gx", "gy", None),
        P(None, "gz", "gx", "gy", None),
        P(),
        P(),
        P(),
    )
    out_specs = (P("gz", "gx", "gy", None), P(None, "gz", "gx", "gy", None))
    return jax.shard_map(
        functools.partial(per_device, sizes),
        mesh=mesh,
        in_specs=in_specs,
        out_specs=out_specs,
        check_vma=False,
    )
```

```python
import functools

import jax
import jax.numpy as jnp
from jax import lax
from jax.experimental import pallas as pl
from jax.experimental.pallas import tpu as pltpu
from jax.sharding import PartitionSpec as P

ITERS = 4
AXES = ("gz", "gx", "gy")
MESH = pl.DeviceIdType.MESH

coulomb_factor = 14.4
cell_edge = 10.0
CHUNK = 64
EDGE = (4.0 * coulomb_factor / cell_edge) ** 0.25
SCALE = EDGE / cell_edge
DEPTH = 64


def kernel(
    sizes, dys,
    offsets_in, type_ids_in, occupied_in, prior_in, electro_in, hardness_in, shielding_in,
    charges, residuals,
    offsets, type_ids, occupied, prior, electro, hardness, shielding,
    first, fields, first_edge, edges, pair, left, right, sums, image, parts, mine,
    in_sem, send_sem, recv_sem, part_send, part_recv,
):
    loads = [
        pltpu.make_async_copy(source, target, in_sem.at[k])
        for k, (source, target) in enumerate(
            zip(
                (offsets_in, type_ids_in, occupied_in, prior_in,
                 electro_in, hardness_in, shielding_in),
                (offsets, type_ids, occupied, prior, electro, hardness, shielding),
            )
        )
    ]
    for load in loads:
        load.start()
    nz, nx, ny = sizes
    cells_x, cells_y, slots = type_ids.shape[1:]
    rows = 2 * cells_y
    geo_rows = 4 * cells_y
    cells = cells_x * cells_y
    devices = nz * nx * ny
    sides = len(dys) - 1
    me_z, me_x, me_y = (lax.axis_index(name) for name in AXES)

    at_x = [lax.rem(me_x + d, nx) for d in range(nx)]
    at_y = [lax.rem(me_y + d, ny) for d in range(ny)]

    def each_peer(action):
        def layer(dz, skip):
            z = lax.rem(me_z + dz, nz)
            for dx in range(nx):
                for dy in range(ny):
                    if not (skip and dx == 0 and dy == 0):
                        action((z, at_x[dx], at_y[dy]), (dz * nx + dx) * ny + dy - 1)

        layer(0, True)
        if nz <= 4:
            for dz in range(1, nz):
                layer(dz, False)
        else:
            pl.loop(1, nz)(lambda dz: layer(dz, False))

    barrier = pltpu.get_barrier_semaphore()
    each_peer(
        lambda peer, slot: pl.semaphore_signal(
            barrier, inc=1, device_id=peer, device_id_type=MESH
        )
    )

    def per_atom(table, ids):
        summed = jnp.zeros(ids.shape, jnp.float32)
        for species in range(table.shape[0]):
            summed = summed + jnp.where(ids == species, table[species], 0.0)
        return summed

    for load in loads:
        load.wait()
    occ, stiff, rhs, x = [], [], [], []

    def ends(values):
        return [values[:1], values[cells_y - 1 : cells_y]]

    for i in range(cells_x):
        ids = type_ids[0, i]
        occ_i = occupied[0, i].astype(jnp.float32)
        radius = per_atom(shielding, ids) * SCALE
        geo = [offsets[c, 0, i] * SCALE for c in range(3)] + [radius * radius]
        first[1, i + 1, :geo_rows] = jnp.concatenate(geo, axis=0)
        stiff_i = per_atom(hardness, ids)
        affinity = per_atom(electro, ids)
        occ.append(jnp.concatenate([occ_i, occ_i], axis=0))
        stiff.append(jnp.concatenate([stiff_i, stiff_i], axis=0))
        rhs.append(jnp.concatenate([-affinity * occ_i, -occ_i], axis=0))
        start = jnp.concatenate([prior[0, 0, i] * occ_i, prior[1, 0, i] * occ_i], axis=0)
        x.append(start)
        first[1, i + 1, geo_rows : geo_rows + rows] = start
        pieces = geo + [start[:cells_y], start[cells_y:]]
        first_edge[i] = jnp.concatenate([end for v in pieces for end in ends(v)], axis=0)

    for edge, slot in ((0, 0), (nz - 1, 2)):

        @pl.when(me_z == edge)
        def _():
            first[slot] = jnp.zeros(first.shape[1:], jnp.float32)
            for k in range(ITERS):
                fields[k, slot] = jnp.zeros(fields.shape[2:], jnp.float32)

    messages = [
        (dz, dx, dy)
        for dx_set, dy_set in (((1, -1), dys[1:]), ((1, -1), (0,)), ((0,), dys[1:]), ((0,), (0,)))
        for dz in (1, -1, 0)
        for dx in dx_set
        for dy in dy_set
        if (dz, dx, dy) != (0, 0, 0)
    ]
    turn_x = {d: lax.rem(me_x + d + nx, nx) for d in (0, 1, -1)}
    turn_y = {d: lax.rem(me_y + d + ny, ny) for d in (0, 1, -1)}

    def each_message(stage, buffer, edge, own_rows, name):
        edge_rows = edge.shape[1]
        for dz, dx, dy in messages:
            source, target, count = {
                0: (0, 1, cells_x),
                1: (cells_x - 1, 0, 1),
                -1: (0, cells_x + 1, 1),
            }[dx]
            if dy == 0:
                src = buffer.at[1, pl.ds(source + 1, count), pl.ds(0, own_rows)]
                span = pl.ds(0, own_rows)
            else:
                src = edge.at[pl.ds(source, count)]
                span = pl.ds(own_rows + (dys.index(dy) - 1) * edge_rows, edge_rows)
            at = (stage, 1 - dz, 1 - dx, dys.index(dy))
            copy = pltpu.make_async_remote_copy(
                src_ref=src,
                dst_ref=buffer.at[1 - dz, pl.ds(target, count), span],
                send_sem=send_sem.at[at],
                recv_sem=recv_sem.at[at],
                device_id=(me_z + dz, turn_x[dx], turn_y[dy]),
                device_id_type=MESH,
            )
            act = getattr(copy, name)
            if dz == 0:
                act()
            else:
                other = me_z + dz
                pl.when((other >= 0) & (other < nz))(act)

    def send(*what):
        each_message(*what, "start")

    def sent(*what):
        each_message(*what, "wait_send")

    def receive(what, plane, side, across):
        stage, buffer, edge, own_rows = what
        edge_rows = edge.shape[1]
        count = cells_x if isinstance(side, int) and side == 1 else 1
        for d in range(len(dys)):
            if (d == 0) == across:
                continue
            rows_in = edge_rows if across else own_rows
            landed = buffer.at[1, pl.ds(1, count), pl.ds(0, rows_in)]
            pltpu.make_async_copy(landed, landed, recv_sem.at[stage, plane, side, d]).wait()

    even = lax.rem(me_z, 2) == 0
    near = jnp.where(even, 2, 0)
    far = 2 - near
    has_far = (me_z + far >= 1) & (me_z + far <= nz)
    has_near = (me_z + near >= 1) & (me_z + near <= nz)
    early = jnp.where(me_x == nx - 1, 0, 2)

    def receive_planes(what, planes, side, across):
        for plane in planes:
            if isinstance(plane, int):
                receive(what, plane, side, across)
            else:
                there = has_near if plane is near else has_far
                pl.when(there)(lambda plane=plane: receive(what, plane, side, across))

    opening = (0, first, first_edge, geo_rows + rows)
    pl.semaphore_wait(barrier, devices - 1)
    send(*opening)

    shape = (slots, slots)
    eye = lax.broadcasted_iota(jnp.int32, shape, 0) == lax.broadcasted_iota(jnp.int32, shape, 1)

    def row_at(q, y, base, own_rows, edge_base, edge_rows):
        if y < 0:
            return own_rows + edge_base + 2 * q + 1
        if y >= cells_y:
            return own_rows + (sides - 1) * edge_rows + edge_base + 2 * q
        return base + q * cells_y + y

    geo_rule = (0, geo_rows + rows, 0, 12)
    start_rule = (geo_rows, geo_rows + rows, 8, 12)
    field_rule = (0, rows, 0, 4)

    def inside(i):
        return [1, 2 - 2 * i] if cells_x == 2 else [1]

    def in_block(j, k):
        return 0 <= j + k - 1 < cells_y

    group = lax.broadcasted_iota(jnp.int32, (8, slots), 0)
    role = lax.rem(group, 4)
    lower = group < 4
    ones = jnp.where(group < 3, 1.0, 0.0)
    nought = jnp.zeros((8, slots), jnp.float32)

    def split(values):
        pieces = []
        for _ in range(3):
            piece = values.astype(jnp.bfloat16).astype(jnp.float32)
            pieces.append(piece)
            values = values - piece
        return pieces

    def place(dz, dx, y):
        start = row_at(0, y, *geo_rule)
        step = cells_y if 0 <= y < cells_y else 2
        four = first[dz, dx, pl.ds(start, 4, stride=step), :]
        both = jnp.concatenate([four, four], axis=0)
        centre_z = (jnp.asarray(dz, jnp.int32).astype(jnp.float32) - 1.5) * EDGE
        centre_x = (jnp.asarray(dx, jnp.int32).astype(jnp.float32) - (1.0 + cells_x / 2)) * EDGE
        centre_y = (y - cells_y / 2) * EDGE
        moved = both + jnp.where(
            role == 0, centre_z, jnp.where(role == 1, centre_x, jnp.where(role == 2, centre_y, 0.0))
        )
        squares = jnp.where((role == 3) | (group > 3), 0.0, moved * moved)
        return moved, jnp.sum(squares, axis=0, keepdims=True), four[3:4]

    def slot_at(dz, dx, y):
        return (dz * (cells_x + 2) + dx) * (cells_y + 2) + y + 1

    def offer(dz, dx, y):
        moved, length, spread = place(dz, dx, y)
        last = jnp.where(lower, length, length + spread)
        p1, p2, p3 = split(jnp.where(role == 3, last, moved))
        to = slot_at(dz, dx, y)
        for half in range(2):
            kept = [
                jnp.where(lower, p, 0.0) if half == 0 else jnp.where(lower, 0.0, p)
                for p in (p1, p2, p3)
            ]
            lines = [kept[q] for q in (0, 1, 2, 0, 1, 0)] + [ones, ones if half else nought]
            right[to, :, half * slots : (half + 1) * slots] = jnp.concatenate(
                lines, axis=0
            ).astype(jnp.bfloat16)

    def take(i, j):
        moved, length, spread = place(1, i + 1, j)
        a1, a2, a3 = split(-2.0 * moved)

        def stacked(value):
            v1, v2, v3 = split(value)
            return jnp.where(group == 0, v1, jnp.where(group == 1, v2, jnp.where(group == 2, v3, 0.0)))

        one = jnp.where(role == 3, 1.0, a1)
        two = jnp.where(role == 3, 0.0, a2)
        three = jnp.where(role == 3, 0.0, a3)
        lines = [one, one, one, two, two, three, stacked(length), stacked(spread)]
        left[i * cells_y + j] = jnp.concatenate(lines, axis=0).T.astype(jnp.bfloat16)

    def couple(i, j, dz, dx, k):
        cell = i * cells_y + j
        other = right[slot_at(dz, i + dx, j + k - 1)]
        for part in range(slots // CHUNK):
            span = pl.ds(part * CHUNK, CHUNK)
            both = jnp.dot(left[cell, span], other, preferred_element_type=jnp.float32)
            squared = jnp.clip(both[:, :slots], 1e-30, EDGE * EDGE)
            apart = squared * lax.rsqrt(squared)
            reach = EDGE - apart
            reach = reach * reach
            pair[cell, (dz * 3 + dx) * 3 + k, span] = (
                reach * reach * (apart + EDGE / 4) * lax.rsqrt(both[:, slots:])
            )

    ends_y = sorted({0, cells_y - 1})

    own = 1
    every = (own, near, far)
    inner, outer = range(cells_y), (-1, cells_y)

    def build(what):
        def plane(dz):
            mirrored = []
            for i in range(cells_x):
                for y in inner:
                    offer(dz, i + 1, y)
            for i in range(cells_x):
                for j in range(cells_y):
                    for dx in inside(i):
                        for k in range(3):
                            if not in_block(j, k):
                                continue
                            if dz is not own or (dx, k) >= (1, 1):
                                couple(i, j, dz, dx, k)
                            else:
                                mirrored.append((i, j, dx, k))
            for i, j, dx, k in mirrored:
                there = (i + dx - 1) * cells_y + j + k - 1
                values = pair[there, (3 + 2 - dx) * 3 + 2 - k]
                pair[i * cells_y + j, (3 + dx) * 3 + k] = values.T

        for i in range(cells_x):
            for j in range(cells_y):
                take(i, j)
        plane(own)

        @pl.loop(0, cells_x)
        def _(i):
            for j in range(cells_y):
                add_pairs(what[1], start_rule, i, j, plane_pairs(own, i, j), True)

        for dz in (near, far):
            receive_planes(what, (dz,), 1, False)
            plane(dz)
        receive_planes(what, every, 1, True)
        for dz in every:
            for i in range(cells_x):
                for y in outer:
                    offer(dz, i + 1, y)
        for i in range(cells_x):
            for dz in every:
                for j in ends_y:
                    for dx in inside(i):
                        for k in range(3):
                            if not in_block(j, k):
                                couple(i, j, dz, dx, k)

    def side_of(turn):
        side = early if turn == 0 else 2 - early
        return side, (cells_x - 1) * (side // 2)

    def accept(what, side, i):
        receive_planes(what, every, side, False)
        receive_planes(what, every, side, True)
        for dz in every:
            for y in (*inner, *outer):
                offer(dz, i + side, y)

    def couple_side(side, i):
        for dz in every:
            for j in range(cells_y):
                for k in range(3):
                    couple(i, j, dz, side, k)

    def add_pairs(buffer, rule, i, j, entries, fresh):
        if fresh:
            total = [jnp.zeros(shape, jnp.float32) for _ in range(2)]
        else:
            total = [sums[i, s * cells_y + j] for s in range(2)]
        for dz, dx, k in entries:
            tile = buffer.at[dz, i + dx]
            block = pair[i * cells_y + j, (dz * 3 + dx) * 3 + k]
            for s in range(2):
                at = row_at(s, j + k - 1, *rule)
                total[s] = total[s] + block * tile[at : at + 1, :]
        for s in range(2):
            sums[i, s * cells_y + j] = total[s]

    def gather(i):
        lines = []
        for row in range(rows):
            column = jnp.sum(sums[i, row], axis=1, keepdims=True)
            lines.append(jnp.sum(jnp.where(eye, column, 0.0), axis=0, keepdims=True))
        image[i] = jnp.concatenate(lines, axis=0)

    def update(field):
        return [occ[i] * (stiff[i] * field[i] + image[i]) for i in range(cells_x)]

    def plane_pairs(dz, i, j):
        return [(dz, dx, k) for dx in inside(i) for k in range(3) if in_block(j, k)]

    def end_pairs(i, j):
        return [
            (dz, dx, k)
            for dz in every for dx in inside(i) for k in range(3)
            if not in_block(j, k)
        ]

    def first_image(what, field):
        buffer, rule = what[1], start_rule

        @pl.loop(0, cells_x)
        def _(i):
            for j in range(cells_y):
                pairs = plane_pairs(near, i, j) + plane_pairs(far, i, j) + end_pairs(i, j)
                add_pairs(buffer, rule, i, j, pairs, False)

        sides = [side_of(turn) for turn in range(2)]
        for side, i in sides:
            accept(what, side, i)
            couple_side(side, i)

        @pl.loop(0, cells_x)
        def _(i):
            side = 2 * i
            for j in range(cells_y):
                pairs = [(dz, side, k) for dz in every for k in range(3)]
                add_pairs(buffer, rule, i, j, pairs, False)
            gather(i)

        return update(field)

    def operate(buffer, rule, field, what):
        def plane(dz, fresh):
            @pl.loop(0, cells_x)
            def _(i):
                for j in range(cells_y):
                    add_pairs(buffer, rule, i, j, plane_pairs(dz, i, j), fresh)

        plane(1, True)
        for dz in (near, far):
            receive_planes(what, (dz,), 1, False)
            plane(dz, False)
        receive_planes(what, every, 1, True)

        @pl.loop(0, cells_x)
        def _(i):
            for j in ends_y:
                add_pairs(buffer, rule, i, j, end_pairs(i, j), False)

        @pl.loop(0, 2)
        def _(turn):
            side = jnp.where(turn == 0, early, 2 - early)
            i = (cells_x - 1) * (side // 2)
            for within in (True, False):
                receive_planes(what, every, side, not within)
                for j in range(cells_y) if within else ends_y:
                    pairs = [(dz, side, k) for dz in every for k in range(3) if in_block(j, k) == within]
                    add_pairs(buffer, rule, i, j, pairs, False)
            gather(i)

        return update(field)

    tile_shape = (rows, slots)
    lane = lax.broadcasted_iota(jnp.int32, tile_shape, 1)
    second = lax.broadcasted_iota(jnp.int32, tile_shape, 0) >= cells_y
    slot_of = lane - jnp.where(second, 8, 0)

    def part_copy(stage, peer, slot):
        return pltpu.make_async_remote_copy(
            src_ref=mine.at[stage],
            dst_ref=parts.at[stage, slot],
            send_sem=part_send.at[stage],
            recv_sem=part_recv.at[stage],
            device_id=peer,
            device_id_type=MESH,
        )

    def start_sums(stage, quantities):
        packed = jnp.zeros(tile_shape, jnp.float32)
        for k, quantity in enumerate(quantities):
            column = jnp.sum(functools.reduce(jnp.add, quantity), axis=1, keepdims=True)
            packed = jnp.where(slot_of == k, column, packed)
        mine[stage] = jnp.sum(packed, axis=0, keepdims=True)
        each_peer(lambda peer, slot: part_copy(stage, peer, slot).start())

    def finish_sums(stage, count):
        everything = parts.at[stage]
        pltpu.make_async_copy(everything, everything, part_recv.at[stage]).wait()
        row = mine[stage] + jnp.sum(parts[stage], axis=0)
        pltpu.make_async_copy(everything, everything, part_send.at[stage]).wait()
        return [
            jnp.where(
                second,
                jnp.broadcast_to(row[:, 8 + k : 9 + k], tile_shape),
                jnp.broadcast_to(row[:, k : k + 1], tile_shape),
            )
            for k in range(count)
        ]

    span = range(cells_x)

    def exchange_and_operate(stage, field, meanwhile=None):
        buffer, edge = fields.at[stage - 1], edges.at[stage - 1]
        for i in span:
            buffer[1, i + 1, :rows] = field[i]
            pieces = [field[i][:cells_y], field[i][cells_y:]]
            edge[i] = jnp.concatenate([end for v in pieces for end in ends(v)], axis=0)
        what = (stage, buffer, edge, rows)
        send(*what)
        if meanwhile is not None:
            meanwhile()
        out = operate(buffer, field_rule, field, what)
        sent(*what)
        return out

    build(opening)
    started = first_image(opening, x)
    sent(*opening)
    r = [rhs[i] - started[i] for i in span]
    w = exchange_and_operate(1, r)

    p = s = z = None
    for stage in range(ITERS):
        quantities = [[r[i] * r[i] for i in span], [w[i] * r[i] for i in span]]
        last = stage == ITERS - 1
        if last:
            quantities += [x, r, p]
        go = functools.partial(start_sums, stage, quantities)
        n = go() if last else exchange_and_operate(stage + 2, w, go)
        found = finish_sums(stage, len(quantities))
        gamma, delta = found[:2]
        if stage == 0:
            beta = None
            alpha = gamma / delta
            p, s, z = r, w, n
        else:
            beta = gamma / gamma_before
            alpha = gamma / (delta - beta * gamma / alpha)
            p = [r[i] + beta * p[i] for i in span]
            s = [w[i] + beta * s[i] for i in span]
            if not last:
                z = [n[i] + beta * z[i] for i in span]
        gamma_before = gamma
        x = [x[i] + alpha * p[i] for i in span]
        r = [r[i] - alpha * s[i] for i in span]
        if not last:
            w = [w[i] - alpha * z[i] for i in span]
    totals = found[2] + alpha * (found[3] + beta * found[4])
    ratio = totals[:cells_y] / totals[cells_y:]
    for i in span:
        charges[0, i] = x[i][:cells_y] - ratio * x[i][cells_y:]
        residuals[0, 0, i] = r[i][:cells_y]
        residuals[1, 0, i] = r[i][cells_y:]


def per_device(sizes, *arrays):
    type_ids = arrays[1]
    cells_x, cells_y, slots = type_ids.shape[1:]
    cells = cells_x * cells_y
    rows = 2 * cells_y
    devices = sizes[0] * sizes[1] * sizes[2]
    dys = (0, 1) if sizes[2] == 2 else (0, 1, -1)
    halo = (3, cells_x + 2)
    sides = len(dys) - 1
    vmem = pl.BlockSpec(memory_space=pltpu.VMEM)
    return pl.pallas_call(
        functools.partial(kernel, sizes, dys),
        out_shape=(
            pltpu.VMEM(type_ids.shape, jnp.float32),
            pltpu.VMEM((2,) + type_ids.shape, jnp.float32),
        ),
        in_specs=[pl.BlockSpec(memory_space=pl.ANY)] * 7,
        out_specs=(vmem, vmem),
        scratch_shapes=[
            *(pltpu.VMEM(array.shape, array.dtype) for array in arrays[:4]),
            *(pltpu.SMEM(array.shape, array.dtype) for array in arrays[4:]),
            pltpu.VMEM(halo + (6 * cells_y + 12 * sides, slots), jnp.float32),
            pltpu.VMEM((ITERS,) + halo + (rows + 4 * sides, slots), jnp.float32),
            pltpu.VMEM((cells_x, 12, slots), jnp.float32),
            pltpu.VMEM((ITERS, cells_x, 4, slots), jnp.float32),
            pltpu.VMEM((cells, 27, slots, slots), jnp.float32),
            pltpu.VMEM((cells, slots, DEPTH), jnp.bfloat16),
            pltpu.VMEM((halo[0] * halo[1] * (cells_y + 2), DEPTH, 2 * slots), jnp.bfloat16),
            pltpu.VMEM((cells_x, rows, slots, slots), jnp.float32),
            pltpu.VMEM((cells_x, rows, slots), jnp.float32),
            pltpu.VMEM((ITERS, devices - 1, 1, slots), jnp.float32),
            pltpu.VMEM((ITERS, 1, slots), jnp.float32),
            pltpu.SemaphoreType.DMA((len(arrays),)),
            pltpu.SemaphoreType.DMA((ITERS + 1, 3, 3, len(dys))),
            pltpu.SemaphoreType.DMA((ITERS + 1, 3, 3, len(dys))),
            pltpu.SemaphoreType.DMA((ITERS,)),
            pltpu.SemaphoreType.DMA((ITERS,)),
        ],
        compiler_params=pltpu.CompilerParams(
            collective_id=0, has_side_effects=True, vmem_limit_bytes=60 * 1024 * 1024
        ),
    )(*arrays)


def solution(mesh):
    sizes = tuple(mesh.shape[name] for name in AXES)
    in_specs = (
        P(None, "gz", "gx", "gy", None),
        P("gz", "gx", "gy", None),
        P("gz", "gx", "gy", None),
        P(None, "gz", "gx", "gy", None),
        P(),
        P(),
        P(),
    )
    out_specs = (P("gz", "gx", "gy", None), P(None, "gz", "gx", "gy", None))
    return jax.shard_map(
        functools.partial(per_device, sizes),
        mesh=mesh,
        in_specs=in_specs,
        out_specs=out_specs,
        check_vma=False,
    )
```

```python
import functools

import jax
import jax.numpy as jnp
from jax import lax
from jax.experimental import pallas as pl
from jax.experimental.pallas import tpu as pltpu
from jax.sharding import PartitionSpec as P

ITERS = 4
AXES = ("gz", "gx", "gy")
MESH = pl.DeviceIdType.MESH

coulomb_factor = 14.4
cell_edge = 10.0
CHUNK = 64
EDGE = (4.0 * coulomb_factor / cell_edge) ** 0.25
SCALE = EDGE / cell_edge
DEPTH = 32


def kernel(
    sizes, dys,
    offsets_in, type_ids_in, occupied_in, prior_in, electro_in, hardness_in, shielding_in,
    charges, residuals,
    offsets, type_ids, occupied, prior, electro, hardness, shielding,
    first, fields, first_edge, edges, pair, left, right, sums, image, parts, mine,
    in_sem, send_sem, recv_sem, part_send, part_recv,
):
    loads = [
        pltpu.make_async_copy(source, target, in_sem.at[k])
        for k, (source, target) in enumerate(
            zip(
                (offsets_in, type_ids_in, occupied_in, prior_in,
                 electro_in, hardness_in, shielding_in),
                (offsets, type_ids, occupied, prior, electro, hardness, shielding),
            )
        )
    ]
    for load in loads:
        load.start()
    nz, nx, ny = sizes
    cells_x, cells_y, slots = type_ids.shape[1:]
    rows = 2 * cells_y
    geo_rows = 4 * cells_y
    cells = cells_x * cells_y
    devices = nz * nx * ny
    sides = len(dys) - 1
    me_z, me_x, me_y = (lax.axis_index(name) for name in AXES)

    at_x = [lax.rem(me_x + d, nx) for d in range(nx)]
    at_y = [lax.rem(me_y + d, ny) for d in range(ny)]

    def each_peer(action):
        def layer(dz, skip):
            z = lax.rem(me_z + dz, nz)
            for dx in (*range(1, nx, 2), *range(2, nx, 2), 0):
                for dy in reversed(range(ny)):
                    if not (skip and dx == 0 and dy == 0):
                        action((z, at_x[dx], at_y[dy]), (dz * nx + dx) * ny + dy - 1)

        if nz <= 4:
            for dz in range(1, nz):
                layer(dz, False)
        else:
            pl.loop(1, nz)(lambda dz: layer(dz, False))
        layer(0, True)

    barrier = pltpu.get_barrier_semaphore()
    each_peer(
        lambda peer, slot: pl.semaphore_signal(
            barrier, inc=1, device_id=peer, device_id_type=MESH
        )
    )

    def per_atom(table, ids):
        summed = jnp.zeros(ids.shape, jnp.float32)
        for species in range(table.shape[0]):
            summed = summed + jnp.where(ids == species, table[species], 0.0)
        return summed

    for load in loads:
        load.wait()
    occ, stiff, rhs, x = [], [], [], []

    def ends(values):
        return [values[:1], values[cells_y - 1 : cells_y]]

    for i in range(cells_x):
        ids = type_ids[0, i]
        occ_i = occupied[0, i].astype(jnp.float32)
        radius = per_atom(shielding, ids) * SCALE
        geo = [offsets[c, 0, i] * SCALE for c in range(3)] + [radius * radius]
        first[1, i + 1, :geo_rows] = jnp.concatenate(geo, axis=0)
        stiff_i = per_atom(hardness, ids)
        affinity = per_atom(electro, ids)
        occ.append(jnp.concatenate([occ_i, occ_i], axis=0))
        stiff.append(jnp.concatenate([stiff_i, stiff_i], axis=0))
        rhs.append(jnp.concatenate([-affinity * occ_i, -occ_i], axis=0))
        start = jnp.concatenate([prior[0, 0, i] * occ_i, prior[1, 0, i] * occ_i], axis=0)
        x.append(start)
        first[1, i + 1, geo_rows : geo_rows + rows] = start
        pieces = geo + [start[:cells_y], start[cells_y:]]
        first_edge[i] = jnp.concatenate([end for v in pieces for end in ends(v)], axis=0)

    for edge, slot in ((0, 0), (nz - 1, 2)):

        @pl.when(me_z == edge)
        def _():
            first[slot] = jnp.zeros(first.shape[1:], jnp.float32)
            for k in range(ITERS):
                fields[k, slot] = jnp.zeros(fields.shape[2:], jnp.float32)

    messages = [
        (dz, dx, dy)
        for dx_set, dy_set in (((1, -1), dys[1:]), ((1, -1), (0,)), ((0,), dys[1:]), ((0,), (0,)))
        for dz in (1, -1, 0)
        for dx in dx_set
        for dy in dy_set
        if (dz, dx, dy) != (0, 0, 0)
    ]
    turn_x = {d: lax.rem(me_x + d + nx, nx) for d in (0, 1, -1)}
    turn_y = {d: lax.rem(me_y + d + ny, ny) for d in (0, 1, -1)}

    def each_message(stage, buffer, edge, own_rows, name):
        edge_rows = edge.shape[1]
        for dz, dx, dy in messages:
            source, target, count = {
                0: (0, 1, cells_x),
                1: (cells_x - 1, 0, 1),
                -1: (0, cells_x + 1, 1),
            }[dx]
            if dy == 0:
                src = buffer.at[1, pl.ds(source + 1, count), pl.ds(0, own_rows)]
                span = pl.ds(0, own_rows)
            else:
                src = edge.at[pl.ds(source, count)]
                span = pl.ds(own_rows + (dys.index(dy) - 1) * edge_rows, edge_rows)
            at = (stage, 1 - dz, 1 - dx, dys.index(dy))
            copy = pltpu.make_async_remote_copy(
                src_ref=src,
                dst_ref=buffer.at[1 - dz, pl.ds(target, count), span],
                send_sem=send_sem.at[at],
                recv_sem=recv_sem.at[at],
                device_id=(me_z + dz, turn_x[dx], turn_y[dy]),
                device_id_type=MESH,
            )
            act = getattr(copy, name)
            if dz == 0:
                act()
            else:
                other = me_z + dz
                pl.when((other >= 0) & (other < nz))(act)

    def send(*what):
        each_message(*what, "start")

    def sent(*what):
        each_message(*what, "wait_send")

    def receive(what, plane, side, across):
        stage, buffer, edge, own_rows = what
        edge_rows = edge.shape[1]
        count = cells_x if isinstance(side, int) and side == 1 else 1
        for d in range(len(dys)):
            if (d == 0) == across:
                continue
            rows_in = edge_rows if across else own_rows
            landed = buffer.at[1, pl.ds(1, count), pl.ds(0, rows_in)]
            pltpu.make_async_copy(landed, landed, recv_sem.at[stage, plane, side, d]).wait()

    even = lax.rem(me_z, 2) == 0
    near = jnp.where(even, 2, 0)
    far = 2 - near
    has_far = (me_z + far >= 1) & (me_z + far <= nz)
    has_near = (me_z + near >= 1) & (me_z + near <= nz)
    early = jnp.where(me_x == nx - 1, 0, 2)

    def receive_planes(what, planes, side, across):
        for plane in planes:
            if isinstance(plane, int):
                receive(what, plane, side, across)
            else:
                there = has_near if plane is near else has_far
                pl.when(there)(lambda plane=plane: receive(what, plane, side, across))

    opening = (0, first, first_edge, geo_rows + rows)
    pl.semaphore_wait(barrier, devices - 1)
    send(*opening)

    shape = (slots, slots)
    eye = lax.broadcasted_iota(jnp.int32, shape, 0) == lax.broadcasted_iota(jnp.int32, shape, 1)

    def row_at(q, y, base, own_rows, edge_base, edge_rows):
        if y < 0:
            return own_rows + edge_base + 2 * q + 1
        if y >= cells_y:
            return own_rows + (sides - 1) * edge_rows + edge_base + 2 * q
        return base + q * cells_y + y

    geo_rule = (0, geo_rows + rows, 0, 12)
    start_rule = (geo_rows, geo_rows + rows, 8, 12)
    field_rule = (0, rows, 0, 4)

    def inside(i):
        return [1, 2 - 2 * i] if cells_x == 2 else [1]

    def in_block(j, k):
        return 0 <= j + k - 1 < cells_y

    group = lax.broadcasted_iota(jnp.int32, (8, slots), 0)
    role = lax.rem(group, 4)
    lower = group < 4

    def split(values):
        pieces = []
        for _ in range(3):
            piece = values.astype(jnp.bfloat16).astype(jnp.float32)
            pieces.append(piece)
            values = values - piece
        return pieces

    def place(dz, dx, y):
        start = row_at(0, y, *geo_rule)
        step = cells_y if 0 <= y < cells_y else 2
        four = first[dz, dx, pl.ds(start, 4, stride=step), :]
        both = jnp.concatenate([four, four], axis=0)
        centre_z = (jnp.asarray(dz, jnp.int32).astype(jnp.float32) - 1.5) * EDGE
        centre_x = (jnp.asarray(dx, jnp.int32).astype(jnp.float32) - (1.0 + cells_x / 2)) * EDGE
        centre_y = (y - cells_y / 2) * EDGE
        moved = both + jnp.where(
            role == 0, centre_z, jnp.where(role == 1, centre_x, jnp.where(role == 2, centre_y, 0.0))
        )
        squares = jnp.where((role == 3) | (group > 3), 0.0, moved * moved)
        return moved, jnp.sum(squares, axis=0, keepdims=True), four[3:4]

    def slot_at(dz, dx, y):
        return (dz * (cells_x + 2) + dx) * (cells_y + 2) + y + 1

    def offer(dz, dx, y):
        moved, length, spread = place(dz, dx, y)
        p1, p2, p3 = split(jnp.where(role == 3, length, moved))
        s1, s2, s3 = split(spread)
        shared = [jnp.where(lower, p1, p2), jnp.where(lower, p3, p1)]
        third = jnp.where(lower, p2, p1)
        ends_of = [
            (0.0, jnp.where(group < 3, 1.0, 0.0)),
            (s3, jnp.where(group < 3, 0.0, jnp.where(group < 6, 1.0, jnp.where(group == 6, s1, s2)))),
        ]
        to = slot_at(dz, dx, y)
        for half, (spare, fourth) in enumerate(ends_of):
            lines = shared + [jnp.where(group == 3, spare, third), fourth]
            right[to, :, half * slots : (half + 1) * slots] = jnp.concatenate(
                lines, axis=0
            ).astype(jnp.bfloat16)

    def take(i, j):
        moved, length, spread = place(1, i + 1, j)
        a1, a2, a3 = split(-2.0 * moved)
        fourth = jnp.ones((8, slots), jnp.float32)
        for at, piece in enumerate(split(length) + split(length + spread)):
            fourth = jnp.where(group == at, piece, fourth)
        last = role == 3
        lines = [
            jnp.where(last, 1.0, a1),
            jnp.where(lower, jnp.where(last, 1.0, a1), jnp.where(last, 0.0, a2)),
            jnp.where(lower, jnp.where(last, 1.0, a2), jnp.where(last, 0.0, a3)),
            fourth,
        ]
        left[i * cells_y + j] = jnp.concatenate(lines, axis=0).T.astype(jnp.bfloat16)

    def couple(i, j, dz, dx, k):
        cell = i * cells_y + j
        other = right[slot_at(dz, i + dx, j + k - 1)]
        for part in range(slots // CHUNK):
            span = pl.ds(part * CHUNK, CHUNK)
            both = jnp.dot(left[cell, span], other, preferred_element_type=jnp.float32)
            squared = jnp.clip(both[:, :slots], 1e-30, EDGE * EDGE)
            apart = squared * lax.rsqrt(squared)
            reach = EDGE - apart
            reach = reach * reach
            pair[cell, (dz * 3 + dx) * 3 + k, span] = (
                reach * reach * (apart + EDGE / 4) * lax.rsqrt(both[:, slots:])
            )

    ends_y = sorted({0, cells_y - 1})

    own = 1
    every = (own, near, far)
    inner, outer = range(cells_y), (-1, cells_y)

    def build(what):
        def plane(dz):
            mirrored = []
            for i in range(cells_x):
                for y in inner:
                    offer(dz, i + 1, y)
            for i in range(cells_x):
                for j in range(cells_y):
                    for dx in inside(i):
                        for k in range(3):
                            if not in_block(j, k):
                                continue
                            if dz is not own or (dx, k) >= (1, 1):
                                couple(i, j, dz, dx, k)
                            else:
                                mirrored.append((i, j, dx, k))
            for i, j, dx, k in mirrored:
                there = (i + dx - 1) * cells_y + j + k - 1
                values = pair[there, (3 + 2 - dx) * 3 + 2 - k]
                pair[i * cells_y + j, (3 + dx) * 3 + k] = values.T

        for i in range(cells_x):
            for j in range(cells_y):
                take(i, j)
        plane(own)

        @pl.loop(0, cells_x)
        def _(i):
            for j in range(cells_y):
                add_pairs(what[1], start_rule, i, j, plane_pairs(own, i, j), True)

        for dz in (near, far):
            receive_planes(what, (dz,), 1, False)
            plane(dz)
        receive_planes(what, every, 1, True)
        for dz in every:
            for i in range(cells_x):
                for y in outer:
                    offer(dz, i + 1, y)
        for i in range(cells_x):
            for dz in every:
                for j in ends_y:
                    for dx in inside(i):
                        for k in range(3):
                            if not in_block(j, k):
                                couple(i, j, dz, dx, k)

    def side_of(turn):
        side = early if turn == 0 else 2 - early
        return side, (cells_x - 1) * (side // 2)

    def accept(what, side, i):
        receive_planes(what, every, side, False)
        receive_planes(what, every, side, True)
        for dz in every:
            for y in (*inner, *outer):
                offer(dz, i + side, y)

    def couple_side(side, i):
        for dz in every:
            for j in range(cells_y):
                for k in range(3):
                    couple(i, j, dz, side, k)

    def add_pairs(buffer, rule, i, j, entries, fresh):
        if fresh:
            total = [jnp.zeros(shape, jnp.float32) for _ in range(2)]
        else:
            total = [sums[i, s * cells_y + j] for s in range(2)]
        for dz, dx, k in entries:
            tile = buffer.at[dz, i + dx]
            block = pair[i * cells_y + j, (dz * 3 + dx) * 3 + k]
            for s in range(2):
                at = row_at(s, j + k - 1, *rule)
                total[s] = total[s] + block * tile[at : at + 1, :]
        for s in range(2):
            sums[i, s * cells_y + j] = total[s]

    def gather(i):
        lines = []
        for row in range(rows):
            column = jnp.sum(sums[i, row], axis=1, keepdims=True)
            lines.append(jnp.sum(jnp.where(eye, column, 0.0), axis=0, keepdims=True))
        image[i] = jnp.concatenate(lines, axis=0)

    def update(field):
        return [occ[i] * (stiff[i] * field[i] + image[i]) for i in range(cells_x)]

    def plane_pairs(dz, i, j):
        return [(dz, dx, k) for dx in inside(i) for k in range(3) if in_block(j, k)]

    def end_pairs(i, j):
        return [
            (dz, dx, k)
            for dz in every for dx in inside(i) for k in range(3)
            if not in_block(j, k)
        ]

    def first_image(what, field):
        buffer, rule = what[1], start_rule

        @pl.loop(0, cells_x)
        def _(i):
            for j in range(cells_y):
                pairs = plane_pairs(near, i, j) + plane_pairs(far, i, j) + end_pairs(i, j)
                add_pairs(buffer, rule, i, j, pairs, False)

        sides = [side_of(turn) for turn in range(2)]
        for side, i in sides:
            accept(what, side, i)
            couple_side(side, i)

        @pl.loop(0, cells_x)
        def _(i):
            side = 2 * i
            for j in range(cells_y):
                pairs = [(dz, side, k) for dz in every for k in range(3)]
                add_pairs(buffer, rule, i, j, pairs, False)
            gather(i)

        return update(field)

    def operate(buffer, rule, field, what):
        def plane(dz, fresh):
            @pl.loop(0, cells_x)
            def _(i):
                for j in range(cells_y):
                    add_pairs(buffer, rule, i, j, plane_pairs(dz, i, j), fresh)

        plane(1, True)
        for dz in (near, far):
            receive_planes(what, (dz,), 1, False)
            plane(dz, False)
        receive_planes(what, every, 1, True)

        @pl.loop(0, cells_x)
        def _(i):
            for j in ends_y:
                add_pairs(buffer, rule, i, j, end_pairs(i, j), False)

        @pl.loop(0, 2)
        def _(turn):
            side = jnp.where(turn == 0, early, 2 - early)
            i = (cells_x - 1) * (side // 2)
            for within in (True, False):
                receive_planes(what, every, side, not within)
                for j in range(cells_y) if within else ends_y:
                    pairs = [(dz, side, k) for dz in every for k in range(3) if in_block(j, k) == within]
                    add_pairs(buffer, rule, i, j, pairs, False)
            gather(i)

        return update(field)

    tile_shape = (rows, slots)
    lane = lax.broadcasted_iota(jnp.int32, tile_shape, 1)
    second = lax.broadcasted_iota(jnp.int32, tile_shape, 0) >= cells_y
    slot_of = lane - jnp.where(second, 8, 0)

    def part_copy(stage, peer, slot):
        return pltpu.make_async_remote_copy(
            src_ref=mine.at[stage],
            dst_ref=parts.at[stage, slot],
            send_sem=part_send.at[stage],
            recv_sem=part_recv.at[stage],
            device_id=peer,
            device_id_type=MESH,
        )

    def start_sums(stage, quantities):
        packed = jnp.zeros(tile_shape, jnp.float32)
        for k, quantity in enumerate(quantities):
            column = jnp.sum(functools.reduce(jnp.add, quantity), axis=1, keepdims=True)
            packed = jnp.where(slot_of == k, column, packed)
        mine[stage] = jnp.sum(packed, axis=0, keepdims=True)
        each_peer(lambda peer, slot: part_copy(stage, peer, slot).start())

    def finish_sums(stage, count):
        everything = parts.at[stage]
        pltpu.make_async_copy(everything, everything, part_recv.at[stage]).wait()
        row = mine[stage] + jnp.sum(parts[stage], axis=0)
        pltpu.make_async_copy(everything, everything, part_send.at[stage]).wait()
        return [
            jnp.where(
                second,
                jnp.broadcast_to(row[:, 8 + k : 9 + k], tile_shape),
                jnp.broadcast_to(row[:, k : k + 1], tile_shape),
            )
            for k in range(count)
        ]

    span = range(cells_x)

    def exchange_and_operate(stage, field, meanwhile=None):
        buffer, edge = fields.at[stage - 1], edges.at[stage - 1]
        for i in span:
            buffer[1, i + 1, :rows] = field[i]
            pieces = [field[i][:cells_y], field[i][cells_y:]]
            edge[i] = jnp.concatenate([end for v in pieces for end in ends(v)], axis=0)
        what = (stage, buffer, edge, rows)
        send(*what)
        if meanwhile is not None:
            meanwhile()
        out = operate(buffer, field_rule, field, what)
        sent(*what)
        return out

    build(opening)
    started = first_image(opening, x)
    sent(*opening)
    r = [rhs[i] - started[i] for i in span]
    w = exchange_and_operate(1, r)

    p = s = z = None
    for stage in range(ITERS):
        quantities = [[r[i] * r[i] for i in span], [w[i] * r[i] for i in span]]
        last = stage == ITERS - 1
        if last:
            quantities += [x, r, p]
        go = functools.partial(start_sums, stage, quantities)
        n = go() if last else exchange_and_operate(stage + 2, w, go)
        found = finish_sums(stage, len(quantities))
        gamma, delta = found[:2]
        if stage == 0:
            beta = None
            alpha = gamma / delta
            p, s, z = r, w, n
        else:
            beta = gamma / gamma_before
            alpha = gamma / (delta - beta * gamma / alpha)
            p = [r[i] + beta * p[i] for i in span]
            s = [w[i] + beta * s[i] for i in span]
            if not last:
                z = [n[i] + beta * z[i] for i in span]
        gamma_before = gamma
        x = [x[i] + alpha * p[i] for i in span]
        r = [r[i] - alpha * s[i] for i in span]
        if not last:
            w = [w[i] - alpha * z[i] for i in span]
    totals = found[2] + alpha * (found[3] + beta * found[4])
    ratio = totals[:cells_y] / totals[cells_y:]
    for i in span:
        charges[0, i] = x[i][:cells_y] - ratio * x[i][cells_y:]
        residuals[0, 0, i] = r[i][:cells_y]
        residuals[1, 0, i] = r[i][cells_y:]


def per_device(sizes, *arrays):
    type_ids = arrays[1]
    cells_x, cells_y, slots = type_ids.shape[1:]
    cells = cells_x * cells_y
    rows = 2 * cells_y
    devices = sizes[0] * sizes[1] * sizes[2]
    dys = (0, 1) if sizes[2] == 2 else (0, 1, -1)
    halo = (3, cells_x + 2)
    sides = len(dys) - 1
    vmem = pl.BlockSpec(memory_space=pltpu.VMEM)
    return pl.pallas_call(
        functools.partial(kernel, sizes, dys),
        out_shape=(
            pltpu.VMEM(type_ids.shape, jnp.float32),
            pltpu.VMEM((2,) + type_ids.shape, jnp.float32),
        ),
        in_specs=[pl.BlockSpec(memory_space=pl.ANY)] * 7,
        out_specs=(vmem, vmem),
        scratch_shapes=[
            *(pltpu.VMEM(array.shape, array.dtype) for array in arrays[:4]),
            *(pltpu.SMEM(array.shape, array.dtype) for array in arrays[4:]),
            pltpu.VMEM(halo + (6 * cells_y + 12 * sides, slots), jnp.float32),
            pltpu.VMEM((ITERS,) + halo + (rows + 4 * sides, slots), jnp.float32),
            pltpu.VMEM((cells_x, 12, slots), jnp.float32),
            pltpu.VMEM((ITERS, cells_x, 4, slots), jnp.float32),
            pltpu.VMEM((cells, 27, slots, slots), jnp.float32),
            pltpu.VMEM((cells, slots, DEPTH), jnp.bfloat16),
            pltpu.VMEM((halo[0] * halo[1] * (cells_y + 2), DEPTH, 2 * slots), jnp.bfloat16),
            pltpu.VMEM((cells_x, rows, slots, slots), jnp.float32),
            pltpu.VMEM((cells_x, rows, slots), jnp.float32),
            pltpu.VMEM((ITERS, devices - 1, 1, slots), jnp.float32),
            pltpu.VMEM((ITERS, 1, slots), jnp.float32),
            pltpu.SemaphoreType.DMA((len(arrays),)),
            pltpu.SemaphoreType.DMA((ITERS + 1, 3, 3, len(dys))),
            pltpu.SemaphoreType.DMA((ITERS + 1, 3, 3, len(dys))),
            pltpu.SemaphoreType.DMA((ITERS,)),
            pltpu.SemaphoreType.DMA((ITERS,)),
        ],
        compiler_params=pltpu.CompilerParams(
            collective_id=0, has_side_effects=True, vmem_limit_bytes=60 * 1024 * 1024
        ),
    )(*arrays)


def solution(mesh):
    sizes = tuple(mesh.shape[name] for name in AXES)
    in_specs = (
        P(None, "gz", "gx", "gy", None),
        P("gz", "gx", "gy", None),
        P("gz", "gx", "gy", None),
        P(None, "gz", "gx", "gy", None),
        P(),
        P(),
        P(),
    )
    out_specs = (P("gz", "gx", "gy", None), P(None, "gz", "gx", "gy", None))
    return jax.shard_map(
        functools.partial(per_device, sizes),
        mesh=mesh,
        in_specs=in_specs,
        out_specs=out_specs,
        check_vma=False,
    )
```
